8 devices in a mesh: prompts: 1 (over z), model: 2 (over y), resp: 4 (over x, core).
Axes of the slice: x: 2, y: 2, z: 1, core: 2. Of those that a mesh axis runs over, the one named last changes fastest.
Arguments:
- x_prompt: bfloat16 [64, 1536], P(('prompts', 'resp'))
- x_resp: bfloat16 [4, 2048, 1536], P(('prompts', 'resp'))
- targets: int32 [4, 2048], P(('prompts', 'resp'))
- resp_lens: int32 [4], P(('prompts', 'resp'))
- attn_gain: float32 [2, 1536], replicated
- w_query: bfloat16 [2, 1536, 12, 128], P(None, None, 'model')
- w_key: bfloat16 [2, 1536, 2, 128], P(None, None, 'model')
- w_value: bfloat16 [2, 1536, 2, 128], P(None, None, 'model')
- w_out: bfloat16 [2, 12, 128, 1536], P(None, 'model')
- mlp_gain: float32 [2, 1536], replicated
- w_gate: bfloat16 [2, 1536, 8960], P(None, None, 'model')
- w_up: bfloat16 [2, 1536, 8960], P(None, None, 'model')
- w_down: bfloat16 [2, 8960, 1536], P(None, 'model')
- final_gain: float32 [1536], replicated
- w_vocab: bfloat16 [1536, 2048], P(None, 'model')
Outputs:
- output: float32 [4, 2048], P(('prompts', 'resp'))
All inputs are finite; a program needn't handle non-finite values.
Results may differ from the reference program's by a relative error of at most 0.00292731.
Values are sent between devices in bfloat16 or wider.
A program may use at most 1 GiB of HBM per device.

```python
import jax
import jax.numpy as jnp
from jax import lax

MODEL_DIM = 1536
NUM_HEADS = 12
KV_HEADS = 2
HEAD_DIM = 128
FFN_DIM = 8960
VOCAB_SIZE = 2048
GROUP_SIZE = 4
PROMPT_ROWS = 16
RESP_LEN = 2048
LAYERS = 2
PROMPT_LEN = GROUP_SIZE * PROMPT_ROWS
EPS = 1e-6
ROPE_BASE = 10000.0


def rms_norm(acts_in, gain_vec):
    acts_f = acts_in.astype(jnp.float32)
    inv_rms = lax.rsqrt(jnp.mean(acts_f * acts_f, axis=-1, keepdims=True) + EPS)
    return (acts_f * inv_rms * gain_vec).astype(jnp.bfloat16)


def rotary(projected, positions):
    half_dim = projected.shape[-1] // 2
    frequency = ROPE_BASE ** (-jnp.arange(half_dim, dtype=jnp.float32) / half_dim)
    angles = positions.astype(jnp.float32)[..., None] * frequency
    cos_part = jnp.cos(angles)[..., None, :]
    sin_part = jnp.sin(angles)[..., None, :]
    lower_half = projected[..., :half_dim]
    upper_half = projected[..., half_dim:]
    return jnp.concatenate([lower_half * cos_part - upper_half * sin_part, upper_half * cos_part + lower_half * sin_part], axis=-1)


def attend(queries, keys, values, query_pos, key_pos):
    tokens = queries.shape[0]
    grouped = queries.reshape(tokens, KV_HEADS, NUM_HEADS // KV_HEADS, HEAD_DIM).astype(jnp.float32)
    scores = jnp.einsum('tkrd,skd->krts', grouped, keys.astype(jnp.float32)) * (HEAD_DIM ** -0.5)
    visible = key_pos[None, :] <= query_pos[:, None]
    scores = jnp.where(visible, scores, -jnp.inf)
    row_max = jnp.max(scores, axis=-1, keepdims=True)
    exp_scores = jnp.exp(scores - row_max)
    row_sum = jnp.moveaxis(jnp.sum(exp_scores, axis=-1), -1, 0)
    mixed = jnp.einsum('krts,skd->tkrd', exp_scores.astype(jnp.bfloat16).astype(jnp.float32), values.astype(jnp.float32))
    return (mixed / row_sum[..., None]).reshape(tokens, NUM_HEADS * HEAD_DIM).astype(jnp.bfloat16)


def setup_inputs(seed: int = 0, part: int = 0) -> dict:
    root_keys = jax.random.split(jax.random.key(seed), 2)
    part_keys = jax.random.split(jax.random.fold_in(root_keys[0], part), 7)
    shared_keys = jax.random.split(root_keys[1], 11)

    def normal_weight(key_in, shape, scale):
        return (jax.random.normal(key_in, shape, jnp.float32) * scale).astype(jnp.bfloat16)

    def gain_draw(key_in, shape):
        return jax.random.uniform(key_in, shape, jnp.float32, 0.25, 1.75)

    topics = jax.random.normal(part_keys[0], (4, 1, MODEL_DIM), jnp.float32)
    prompt_noise = jax.random.normal(part_keys[1], (4, PROMPT_LEN // 4, MODEL_DIM), jnp.float32)
    x_prompt = (0.6 * topics + 0.3 * prompt_noise).reshape(PROMPT_LEN, MODEL_DIM).astype(jnp.bfloat16)
    resp_topics = jax.random.normal(part_keys[2], (GROUP_SIZE, 1, MODEL_DIM), jnp.float32)
    resp_noise = jax.random.normal(part_keys[3], (GROUP_SIZE, RESP_LEN, MODEL_DIM), jnp.float32)
    x_resp = (0.6 * resp_topics + 0.3 * resp_noise).astype(jnp.bfloat16)
    targets = jax.random.randint(part_keys[4], (GROUP_SIZE, RESP_LEN), 0, VOCAB_SIZE, dtype=jnp.int32)
    targets = targets.at[0, 0].set(0).at[0, 1].set(VOCAB_SIZE - 1)
    drawn_lens = jax.random.randint(part_keys[5], (GROUP_SIZE,), RESP_LEN // 8, RESP_LEN + 1, dtype=jnp.int32)
    full_slot = jax.random.randint(part_keys[6], (), 0, GROUP_SIZE, dtype=jnp.int32)
    resp_lens = jnp.where(jnp.arange(GROUP_SIZE) == full_slot, RESP_LEN, drawn_lens).astype(jnp.int32)
    return {
        'x_prompt': x_prompt,
        'x_resp': x_resp,
        'targets': targets,
        'resp_lens': resp_lens,
        'attn_gain': gain_draw(shared_keys[0], (LAYERS, MODEL_DIM)),
        'w_query': normal_weight(shared_keys[1], (LAYERS, MODEL_DIM, NUM_HEADS, HEAD_DIM), MODEL_DIM ** -0.5),
        'w_key': normal_weight(shared_keys[2], (LAYERS, MODEL_DIM, KV_HEADS, HEAD_DIM), MODEL_DIM ** -0.5),
        'w_value': normal_weight(shared_keys[3], (LAYERS, MODEL_DIM, KV_HEADS, HEAD_DIM), MODEL_DIM ** -0.5),
        'w_out': normal_weight(shared_keys[4], (LAYERS, NUM_HEADS, HEAD_DIM, MODEL_DIM), (NUM_HEADS * HEAD_DIM) ** -0.5),
        'mlp_gain': gain_draw(shared_keys[5], (LAYERS, MODEL_DIM)),
        'w_gate': normal_weight(shared_keys[6], (LAYERS, MODEL_DIM, FFN_DIM), MODEL_DIM ** -0.5),
        'w_up': normal_weight(shared_keys[7], (LAYERS, MODEL_DIM, FFN_DIM), MODEL_DIM ** -0.5),
        'w_down': normal_weight(shared_keys[8], (LAYERS, FFN_DIM, MODEL_DIM), FFN_DIM ** -0.5),
        'final_gain': gain_draw(shared_keys[9], (MODEL_DIM,)),
        'w_vocab': normal_weight(shared_keys[10], (MODEL_DIM, VOCAB_SIZE), 2.0 * MODEL_DIM ** -0.5),
    }


def reference(x_prompt, x_resp, targets, resp_lens, attn_gain, w_query, w_key, w_value, w_out, mlp_gain, w_gate, w_up, w_down, final_gain, w_vocab):
    prompt_pos = jnp.arange(PROMPT_LEN)
    resp_pos = PROMPT_LEN + jnp.arange(RESP_LEN)
    key_pos = jnp.concatenate([prompt_pos, resp_pos])

    def project(hidden, weight, heads):
        flat = jnp.dot(hidden, weight.reshape(MODEL_DIM, heads * HEAD_DIM), preferred_element_type=jnp.float32)
        return flat.reshape(hidden.shape[0], heads, HEAD_DIM)

    def key_value(hidden, layer_idx, positions):
        keys = rotary(project(hidden, w_key[layer_idx], KV_HEADS), positions).astype(jnp.bfloat16)
        values = project(hidden, w_value[layer_idx], KV_HEADS).astype(jnp.bfloat16)
        return keys, values

    def query_proj(hidden, layer_idx, positions):
        return rotary(project(hidden, w_query[layer_idx], NUM_HEADS), positions).astype(jnp.bfloat16)

    def finish(residual, mixed, layer_idx):
        attn_out = jnp.dot(mixed, w_out[layer_idx].reshape(NUM_HEADS * HEAD_DIM, MODEL_DIM), preferred_element_type=jnp.float32)
        residual = (residual.astype(jnp.float32) + attn_out).astype(jnp.bfloat16)
        hidden = rms_norm(residual, mlp_gain[layer_idx])
        gate = jnp.dot(hidden, w_gate[layer_idx], preferred_element_type=jnp.float32)
        up_proj = jnp.dot(hidden, w_up[layer_idx], preferred_element_type=jnp.float32)
        inner = (jax.nn.silu(gate) * up_proj).astype(jnp.bfloat16)
        down_out = jnp.dot(inner, w_down[layer_idx], preferred_element_type=jnp.float32)
        return (residual.astype(jnp.float32) + down_out).astype(jnp.bfloat16)

    residual = x_prompt
    prompt_cache = []
    for layer_idx in range(LAYERS):
        hidden = rms_norm(residual, attn_gain[layer_idx])
        keys, values = key_value(hidden, layer_idx, prompt_pos)
        prompt_cache.append((keys, values))
        if layer_idx < LAYERS - 1:
            blocks = query_proj(hidden, layer_idx, prompt_pos).reshape(GROUP_SIZE, PROMPT_ROWS, NUM_HEADS, HEAD_DIM)
            block_pos = prompt_pos.reshape(GROUP_SIZE, PROMPT_ROWS)
            mixed = lax.map(lambda block_args: attend(block_args[0], keys, values, block_args[1], prompt_pos), (blocks, block_pos))
            residual = finish(residual, mixed.reshape(PROMPT_LEN, NUM_HEADS * HEAD_DIM), layer_idx)

    def one_response(resp_args):
        residual_r, target_row, length = resp_args
        for layer_idx in range(LAYERS):
            hidden = rms_norm(residual_r, attn_gain[layer_idx])
            keys, values = key_value(hidden, layer_idx, resp_pos)
            queries = query_proj(hidden, layer_idx, resp_pos)
            all_keys = jnp.concatenate([prompt_cache[layer_idx][0], keys], axis=0)
            all_values = jnp.concatenate([prompt_cache[layer_idx][1], values], axis=0)
            mixed = attend(queries, all_keys, all_values, resp_pos, key_pos)
            residual_r = finish(residual_r, mixed, layer_idx)
        logits = jnp.dot(rms_norm(residual_r, final_gain), w_vocab, preferred_element_type=jnp.float32)
        picked = jnp.take_along_axis(logits, target_row[:, None], axis=-1)[:, 0]
        log_probs = picked - jax.nn.logsumexp(logits, axis=-1)
        return jnp.where(jnp.arange(RESP_LEN) < length, log_probs, 0.0)

    return lax.map(one_response, (x_resp, targets, resp_lens))
```

```python
import functools

import jax
import jax.numpy as jnp
from jax import lax
from jax.experimental import pallas as pl
from jax.experimental.pallas import tpu as pltpu
from jax.sharding import PartitionSpec as P

EPS = 1e-6
ROPE_BASE = 10000.0
HEAD = 128
BLOCK = 352
OWNED = ((0, 3, 5), (1, 2, 4))


def rms_norm(acts_in, gain_vec):
    acts_f = acts_in.astype(jnp.float32)
    inv_rms = lax.rsqrt(jnp.mean(acts_f * acts_f, axis=-1, keepdims=True) + EPS)
    return (acts_f * inv_rms * gain_vec).astype(jnp.bfloat16)


def dot(a, b):
    return jnp.dot(a, b, preferred_element_type=jnp.float32)


def attention_kernel(num_blocks, heads, ids_ref, q_ref, k_ref, v_ref, o_ref):
    block_id = ids_ref[pl.program_id(1)]
    rows = q_ref.shape[0]

    def body(i):
        first = i * rows
        low = first // 128 * 128
        high = min(-(-(first + rows) // 128) * 128, k_ref.shape[0])
        row = first + lax.broadcasted_iota(jnp.int32, (rows, high - low), 0)
        col = low + lax.broadcasted_iota(jnp.int32, (rows, high - low), 1)
        seen = col <= row
        for h in range(heads):
            q = q_ref[:, h * HEAD:(h + 1) * HEAD]
            nt = (((1,), (1,)), ((), ()))
            s_hi = lax.dot_general(q, k_ref[low:high, :], nt, preferred_element_type=jnp.float32)
            s_hi = jnp.where(seen, s_hi, -jnp.inf)
            m = jnp.max(s_hi, axis=-1, keepdims=True)
            if low:
                s_lo = lax.dot_general(q, k_ref[:low, :], nt, preferred_element_type=jnp.float32)
                m = jnp.maximum(m, jnp.max(s_lo, axis=-1, keepdims=True))
            scale = HEAD ** -0.5
            p_hi = jnp.exp((s_hi - m) * scale)
            total = jnp.sum(p_hi, axis=-1, keepdims=True)
            out = dot(p_hi.astype(jnp.bfloat16), v_ref[low:high, :])
            if low:
                p_lo = jnp.exp((s_lo - m) * scale)
                total = total + jnp.sum(p_lo, axis=-1, keepdims=True)
                out = out + dot(p_lo.astype(jnp.bfloat16), v_ref[:low, :])
            o_ref[:, h * HEAD:(h + 1) * HEAD] = (out / total).astype(jnp.bfloat16)

    for i in range(num_blocks):
        pl.when(block_id == i)(functools.partial(body, i))


def attention(ids, q, k, v, num_blocks):
    rows, width = q.shape
    per_step = 2
    n = rows // BLOCK
    keys = k.shape[0]
    spec = pltpu.PrefetchScalarGridSpec(
        num_scalar_prefetch=1,
        grid=(width // (per_step * HEAD), n),
        in_specs=[
            pl.BlockSpec((BLOCK, per_step * HEAD), lambda h, b, ids: (b, h)),
            pl.BlockSpec((keys, HEAD), lambda h, b, ids: (0, 0)),
            pl.BlockSpec((keys, HEAD), lambda h, b, ids: (0, 0)),
        ],
        out_specs=pl.BlockSpec((BLOCK, per_step * HEAD), lambda h, b, ids: (b, h)),
    )
    return pl.pallas_call(
        functools.partial(attention_kernel, num_blocks, per_step),
        grid_spec=spec,
        out_shape=jax.ShapeDtypeStruct((rows, width), jnp.bfloat16),
        compiler_params=pltpu.CompilerParams(
            dimension_semantics=("arbitrary", "arbitrary"), vmem_limit_bytes=48 * 2**20),
        cost_estimate=pl.CostEstimate(
            flops=int(rows * keys * width * 4), bytes_accessed=rows * width * 4 + keys * HEAD * 4,
            transcendentals=rows * keys * width // HEAD // 2),
    )(ids, q, k, v)


def solution(mesh):
    groups = mesh.shape['resp']
    row_axes = ('prompts', 'resp')
    head_spec = P(None, None, 'model', None)
    in_specs = (P(row_axes, None), P(row_axes, None, None), P(row_axes, None), P(row_axes), P(None, None), head_spec, head_spec, head_spec, P(None, 'model', None, None), P(None, None), P(None, None, 'model'), P(None, None, 'model'), P(None, 'model', None), P(None), P(None, 'model'))
    across = [(0, 1), (1, 0)]
    core = [(i, i ^ 1) for i in range(groups)]
    chip = [(i, i ^ 2) for i in range(groups)]

    def swap(a):
        return lax.ppermute(a, 'model', across)

    def spread(a):
        far = lax.ppermute(a, 'resp', chip)
        return [a, lax.ppermute(a, 'resp', core), far, lax.ppermute(far, 'resp', core)]

    def device_step(x_prompt, x_resp, targets, resp_lens, attn_gain, w_query, w_key, w_value, w_out, mlp_gain, w_gate, w_up, w_down, final_gain, w_vocab):
        me = lax.axis_index('resp')
        side = lax.axis_index('model')
        resp_len = x_resp.shape[1]
        dim = x_resp.shape[2]
        prompt_len = x_prompt.shape[0] * groups
        tokens = prompt_len + resp_len
        blocks = tokens // BLOCK
        keys_pad = -(-tokens // 128) * 128
        q_width = w_query.shape[2] * HEAD
        ffn = w_gate.shape[2]
        vocab = w_vocab.shape[1]

        def in_order(pieces):
            stack = jnp.stack(pieces)
            return jnp.concatenate([lax.dynamic_index_in_dim(stack, me ^ j, 0, keepdims=False) for j in range(groups)], axis=0)

        def quarter(w, axis):
            size = w.shape[axis] // groups
            return lax.dynamic_slice_in_dim(w, me * size, size, axis)

        def own_qkv(l):
            return jnp.concatenate([w_query[l].reshape(dim, q_width), w_key[l].reshape(dim, HEAD), w_value[l].reshape(dim, HEAD)], axis=1)

        def own_out(l):
            return w_out[l].reshape(q_width, dim)

        def fetch_rows(w):
            return in_order(spread(swap(quarter(w, 0))))

        qkv_own = [own_qkv(0), own_qkv(1)]
        out_own = [own_out(0), own_out(1)]
        qkv_far0 = fetch_rows(qkv_own[0])
        out_far0 = fetch_rows(out_own[0])

        prompt = in_order(spread(x_prompt))
        x = jnp.concatenate([prompt, x_resp[0]], axis=0)

        half = HEAD // 2
        frequency = ROPE_BASE ** (-jnp.arange(half, dtype=jnp.float32) / half)
        angles = jnp.arange(tokens).astype(jnp.float32)[:, None] * frequency
        cos_all, sin_all = jnp.cos(angles), jnp.sin(angles)

        def rotary(a, cos_part, sin_part):
            a = a.reshape(a.shape[0], -1, HEAD)
            low, high = a[..., :half], a[..., half:]
            c, s = cos_part[:, None, :], sin_part[:, None, :]
            out = jnp.concatenate([low * c - high * s, high * c + low * s], axis=-1).astype(jnp.bfloat16)
            return out.reshape(a.shape[0], -1)

        def project(h, w, cos_part, sin_part):
            f = dot(h, w)
            qk = rotary(f[:, :q_width + HEAD], cos_part, sin_part)
            return qk[:, :q_width], qk[:, q_width:], f[:, q_width + HEAD:].astype(jnp.bfloat16)

        def pad(a):
            return jnp.pad(a, ((0, keys_pad - tokens), (0, 0)))

        h = rms_norm(x, attn_gain[0])
        ids_all = jnp.arange(blocks, dtype=jnp.int32)
        q, k, v = project(h, qkv_own[0], cos_all, sin_all)
        mixed_own = attention(ids_all, q, pad(k), pad(v), blocks)
        q, k, v = project(h, qkv_far0, cos_all, sin_all)
        mixed_far = attention(ids_all, q, pad(k), pad(v), blocks)
        x = (x.astype(jnp.float32) + (dot(mixed_own, out_own[0]) + dot(mixed_far, out_far0))).astype(jnp.bfloat16)

        owned = jnp.array(OWNED, jnp.int32)
        mine = owned[side]
        theirs = owned[1 - side]

        def take(a, ids):
            return jnp.concatenate([lax.dynamic_slice_in_dim(a, ids[i] * BLOCK, BLOCK, 0) for i in range(ids.shape[0])], axis=0)

        u = rms_norm(x, mlp_gain[0])

        def mlp(rows, gate_w, up_w, down_w):
            inner = (jax.nn.silu(dot(rows, gate_w)) * dot(rows, up_w)).astype(jnp.bfloat16)
            return dot(inner, down_w)

        u_theirs = take(u, theirs)
        got = []
        for i in range(theirs.shape[0]):
            part = mlp(u_theirs[i * BLOCK:(i + 1) * BLOCK], w_gate[0], w_up[0], w_down[0])
            got.append(swap(part))
        part_mine = mlp(take(u, mine), w_gate[0], w_up[0], w_down[0])
        x = (take(x, mine).astype(jnp.float32) + (part_mine + jnp.concatenate(got, axis=0))).astype(jnp.bfloat16)

        qkv_far1 = fetch_rows(qkv_own[1])
        out_far1 = fetch_rows(out_own[1])
        cos_own, sin_own = take(cos_all, mine), take(sin_all, mine)
        h = rms_norm(x, attn_gain[1])
        q_own, k_own, v_own = project(h, qkv_own[1], cos_own, sin_own)
        q_far, k_far, v_far = project(h, qkv_far1, cos_own, sin_own)
        kv_mine = jnp.concatenate([k_own, v_own, k_far, v_far], axis=1)
        kv_sent = jnp.concatenate([k_far, v_far, k_own, v_own], axis=1)
        kv_got = swap(kv_sent)

        def merge(own_part, far_part):
            def split(a):
                return [a[i * BLOCK:(i + 1) * BLOCK] for i in range(a.shape[0] // BLOCK)]
            a, b = split(own_part), split(far_part)
            order = [[None] * blocks, [None] * blocks]
            for s in range(2):
                for i, blk in enumerate(OWNED[s]):
                    order[s][blk] = a[i]
                for i, blk in enumerate(OWNED[1 - s]):
                    order[s][blk] = b[i]
            return jnp.concatenate([jnp.where(side == 0, p0, p1) for p0, p1 in zip(*order)], axis=0)

        kv = pad(merge(kv_mine, kv_got))
        mixed_own = attention(mine, q_own, kv[:, :HEAD], kv[:, HEAD:2 * HEAD], blocks)
        mixed_far = attention(mine, q_far, kv[:, 2 * HEAD:3 * HEAD], kv[:, 3 * HEAD:], blocks)
        x = (x.astype(jnp.float32) + (dot(mixed_own, out_own[1]) + dot(mixed_far, out_far1))).astype(jnp.bfloat16)

        u = rms_norm(x, mlp_gain[1])
        total = mlp(u, w_gate[1], w_up[1], w_down[1])
        base = me * (ffn // groups)
        done = 0
        for size in (256, 256, 256, 256, 96):
            at = base + done
            gate_up = jnp.concatenate([lax.dynamic_slice_in_dim(w_gate[1], at, size, 1), lax.dynamic_slice_in_dim(w_up[1], at, size, 1)], axis=1)
            down = lax.dynamic_slice_in_dim(w_down[1], at, size, 0)
            gate_up = spread(swap(gate_up))
            down = spread(swap(down))
            total = total + mlp(u, jnp.concatenate([g[:, :size] for g in gate_up], axis=1), jnp.concatenate([g[:, size:] for g in gate_up], axis=1), jnp.concatenate(down, axis=0))
            done += size
        x = (x.astype(jnp.float32) + total).astype(jnp.bfloat16)

        vocab_far = spread(swap(quarter(w_vocab, 1)))
        logits = dot(rms_norm(x, final_gain), jnp.concatenate([w_vocab] + vocab_far, axis=1))
        piece = vocab // groups
        ids = [side * vocab + jnp.arange(vocab)] + [(1 - side) * vocab + (me ^ j) * piece + jnp.arange(piece) for j in range(groups)]
        vocab_ids = jnp.concatenate(ids)
        padded_targets = jnp.concatenate([jnp.zeros((prompt_len,), targets.dtype), targets[0]])[:, None]
        target_own = take(padded_targets, mine)
        row_max = jnp.max(logits, axis=-1)
        exp_total = jnp.sum(jnp.exp(logits - row_max[:, None]), axis=-1)
        picked = jnp.sum(jnp.where(vocab_ids[None, :] == target_own, logits, 0.0), axis=-1)
        log_probs = picked - row_max - jnp.log(exp_total)
        log_probs = merge(log_probs, swap(log_probs))[prompt_len:]
        log_probs = jnp.where(jnp.arange(resp_len) < resp_lens[0], log_probs, 0.0)
        return log_probs[None, :]

    return jax.shard_map(device_step, mesh=mesh, in_specs=in_specs, out_specs=P(row_axes, None), check_vma=False)
```

```python
import functools

import jax
import jax.numpy as jnp
from jax import lax
from jax.experimental import pallas as pl
from jax.experimental.pallas import tpu as pltpu
from jax.sharding import PartitionSpec as P


EPS = 1e-6
ROPE_BASE = 10000.0
HEAD = 128
BLOCK = 352
TILE = 896
OWNED = ((0, 3, 5), (1, 2, 4))
CHUNKS = (384, 256, 256, 128)
TAIL = 128
MIB = 2**20


def dot(a, b):
    return jnp.dot(a, b, preferred_element_type=jnp.float32)


def normalize(x, gain):
    f = x.astype(jnp.float32)
    inv_rms = lax.rsqrt(jnp.mean(f * f, axis=-1, keepdims=True) + EPS)
    return (f * inv_rms * gain).astype(jnp.bfloat16)


def params(vmem_mib):
    return pltpu.CompilerParams(dimension_semantics=("arbitrary",), vmem_limit_bytes=vmem_mib * MIB)


def cost(flops, data):
    return pl.CostEstimate(flops=int(flops), bytes_accessed=int(data), transcendentals=0)


def project_kernel(q_width, ids_ref, x_ref, gain_ref, w_ref, cos_ref, sin_ref, q_ref, k_ref, v_ref):
    h = normalize(x_ref[...], gain_ref[...])
    f = dot(h, w_ref[...])
    cos_part, sin_part = cos_ref[...], sin_ref[...]
    for i in range(q_width // HEAD + 1):
        a = f[:, i * HEAD:(i + 1) * HEAD]
        r = (a * cos_part + pltpu.roll(a, HEAD // 2, 1) * sin_part).astype(jnp.bfloat16)
        if i < q_width // HEAD:
            q_ref[:, i * HEAD:(i + 1) * HEAD] = r
        else:
            k_ref[...] = r
    v_ref[...] = f[:, q_width + HEAD:].astype(jnp.bfloat16)


def project(ids, x, gain, w, cos_all, sin_all, key_rows):
    rows, dim = x.shape
    width = w.shape[1]
    q_width = width - 2 * HEAD
    row = lambda b, ids: (b, 0)
    whole = lambda b, ids: (0, 0)
    table = lambda b, ids: (ids[b], 0)
    return pl.pallas_call(
        functools.partial(project_kernel, q_width),
        grid_spec=pltpu.PrefetchScalarGridSpec(
            num_scalar_prefetch=1,
            grid=(rows // BLOCK,),
            in_specs=[
                pl.BlockSpec((BLOCK, dim), row),
                pl.BlockSpec((1, dim), whole),
                pl.BlockSpec((dim, width), whole),
                pl.BlockSpec((BLOCK, HEAD), table),
                pl.BlockSpec((BLOCK, HEAD), table),
            ],
            out_specs=[pl.BlockSpec((BLOCK, q_width), row), pl.BlockSpec((BLOCK, HEAD), row), pl.BlockSpec((BLOCK, HEAD), row)],
        ),
        out_shape=[
            jax.ShapeDtypeStruct((rows, q_width), jnp.bfloat16),
            jax.ShapeDtypeStruct((key_rows, HEAD), jnp.bfloat16),
            jax.ShapeDtypeStruct((key_rows, HEAD), jnp.bfloat16),
        ],
        compiler_params=params(40),
        cost_estimate=cost(2 * rows * dim * width, 2 * (rows * dim + dim * width + rows * width)),
    )(ids, x, gain[None, :], w, cos_all, sin_all)


def attention_kernel(num_blocks, heads, ids_ref, q_ref, k_ref, v_ref, o_ref):
    block_id = ids_ref[pl.program_id(1)]
    rows = q_ref.shape[0]
    nt = (((1,), (1,)), ((), ()))
    scale = HEAD ** -0.5

    def body(i):
        first = i * rows
        low = first // 128 * 128
        high = -(-(first + rows) // 128) * 128
        row = first + lax.broadcasted_iota(jnp.int32, (rows, high - low), 0)
        col = low + lax.broadcasted_iota(jnp.int32, (rows, high - low), 1)
        seen = col <= row
        v_hi = v_ref[low:high, :]
        if high > num_blocks * rows:
            at = low + lax.broadcasted_iota(jnp.int32, v_hi.shape, 0)
            v_hi = jnp.where(at < num_blocks * rows, v_hi, jnp.zeros_like(v_hi))
        for h in range(heads):
            q = q_ref[:, h * HEAD:(h + 1) * HEAD]
            s_hi = lax.dot_general(q, k_ref[low:high, :], nt, preferred_element_type=jnp.float32)
            s_hi = jnp.where(seen, s_hi, -jnp.inf)
            m = jnp.max(s_hi, axis=-1, keepdims=True)
            if low:
                s_lo = lax.dot_general(q, k_ref[:low, :], nt, preferred_element_type=jnp.float32)
                m = jnp.maximum(m, jnp.max(s_lo, axis=-1, keepdims=True))
            p_hi = jnp.exp((s_hi - m) * scale)
            total = jnp.sum(p_hi, axis=-1, keepdims=True)
            out = dot(p_hi.astype(jnp.bfloat16), v_hi)
            if low:
                p_lo = jnp.exp((s_lo - m) * scale)
                total = total + jnp.sum(p_lo, axis=-1, keepdims=True)
                out = out + dot(p_lo.astype(jnp.bfloat16), v_ref[:low, :])
            o_ref[:, h * HEAD:(h + 1) * HEAD] = (out / total).astype(jnp.bfloat16)

    for i in range(num_blocks):
        pl.when(block_id == i)(functools.partial(body, i))


def attention(ids, q, k, v, num_blocks):
    rows, width = q.shape
    per_step = 2
    keys = k.shape[0]
    return pl.pallas_call(
        functools.partial(attention_kernel, num_blocks, per_step),
        grid_spec=pltpu.PrefetchScalarGridSpec(
            num_scalar_prefetch=1,
            grid=(width // (per_step * HEAD), rows // BLOCK),
            in_specs=[
                pl.BlockSpec((BLOCK, per_step * HEAD), lambda h, b, ids: (b, h)),
                pl.BlockSpec((keys, HEAD), lambda h, b, ids: (0, 0)),
                pl.BlockSpec((keys, HEAD), lambda h, b, ids: (0, 0)),
            ],
            out_specs=pl.BlockSpec((BLOCK, per_step * HEAD), lambda h, b, ids: (b, h)),
        ),
        out_shape=jax.ShapeDtypeStruct((rows, width), jnp.bfloat16),
        compiler_params=pltpu.CompilerParams(
            dimension_semantics=("arbitrary", "arbitrary"), vmem_limit_bytes=40 * MIB),
        cost_estimate=cost(8 * rows * keys * width, rows * width * 4 + keys * HEAD * 4),
    )(ids, q, k, v)


def output_kernel(x_ref, a_ref, b_ref, wa_ref, wb_ref, gain_ref, x_out, u_out):
    total = dot(a_ref[...], wa_ref[0]) + dot(b_ref[...], wb_ref[...])
    x = (x_ref[...].astype(jnp.float32) + total).astype(jnp.bfloat16)
    x_out[...] = x
    u_out[...] = normalize(x, gain_ref[...])


def project_out(layer, x, a, b, w_own, w_far, gain):
    rows, dim = x.shape
    width = a.shape[1]
    row = lambda i: (i, 0)
    return pl.pallas_call(
        output_kernel,
        grid=(rows // BLOCK,),
        in_specs=[
            pl.BlockSpec((BLOCK, dim), row),
            pl.BlockSpec((BLOCK, width), row),
            pl.BlockSpec((BLOCK, width), row),
            pl.BlockSpec((1, width, dim), lambda i: (layer, 0, 0)),
            pl.BlockSpec((width, dim), lambda i: (0, 0)),
            pl.BlockSpec((1, dim), lambda i: (0, 0)),
        ],
        out_specs=[pl.BlockSpec((BLOCK, dim), row), pl.BlockSpec((BLOCK, dim), row)],
        out_shape=[jax.ShapeDtypeStruct((rows, dim), jnp.bfloat16)] * 2,
        compiler_params=params(40),
        cost_estimate=cost(4 * rows * dim * width, 6 * rows * dim + 8 * width * dim),
    )(x, a, b, w_own, w_far, gain[None, :])


def mlp_rows(u_ref, out_ref, gate, up, down, fresh):
    def rows(i, _):
        at = pl.ds(pl.multiple_of(i * BLOCK, BLOCK), BLOCK)
        u = u_ref[at, :]
        g = dot(u, gate())
        inner = (jax.nn.silu(g) * dot(u, up())).astype(jnp.bfloat16)
        part = dot(inner, down())
        if fresh is None:
            out_ref[at, :] += part
        else:
            out_ref[at, :] = jnp.where(fresh, part, out_ref[at, :] + part)
        return 0

    n = u_ref.shape[0] // BLOCK
    if n == 1:
        rows(0, 0)
    else:
        lax.fori_loop(0, n, rows, 0)


def mlp_kernel(ids_ref, u_ref, gate_ref, up_ref, down_ref, out_ref):
    first = pl.program_id(0) == 0

    @pl.when(first)
    def _():
        out_ref[...] = jnp.zeros_like(out_ref)

    mlp_rows(u_ref, out_ref, lambda: gate_ref[0], lambda: up_ref[0], lambda: down_ref[0], None)


def mlp_own(layer, ids, u, rows, w_gate, w_up, w_down):
    dim = u.shape[1]
    ffn = w_gate.shape[2]
    return pl.pallas_call(
        mlp_kernel,
        grid_spec=pltpu.PrefetchScalarGridSpec(
            num_scalar_prefetch=1,
            grid=(ffn // TILE,),
            in_specs=[
                pl.BlockSpec((rows, dim), lambda j, ids: (ids[0], 0)),
                pl.BlockSpec((1, dim, TILE), lambda j, ids: (layer, 0, j)),
                pl.BlockSpec((1, dim, TILE), lambda j, ids: (layer, 0, j)),
                pl.BlockSpec((1, TILE, dim), lambda j, ids: (layer, j, 0)),
            ],
            out_specs=pl.BlockSpec((rows, dim), lambda j, ids: (0, 0)),
        ),
        out_shape=jax.ShapeDtypeStruct((rows, dim), jnp.float32),
        compiler_params=params(56),
        cost_estimate=cost(6 * rows * dim * ffn, 6 * dim * ffn + 6 * rows * dim),
    )(ids, u, w_gate, w_up, w_down)


def mlp_pieces_kernel(n, u_ref, acc_ref, *refs):
    wide, tall = refs[:n], refs[n:2 * n]
    out_ref, wide_v, tall_v, sems = refs[2 * n:]
    size = wide_v.shape[2] // 2
    copies = []
    for j in range(n):
        pair = (pltpu.make_async_copy(wide[j], wide_v.at[j], sems.at[2 * j]), pltpu.make_async_copy(tall[j], tall_v.at[j], sems.at[2 * j + 1]))
        for c in pair:
            c.start()
        copies.append(pair)
    out_ref[...] = acc_ref[...]
    for j in range(n):
        for c in copies[j]:
            c.wait()
        mlp_rows(u_ref, out_ref, lambda: wide_v[j, :, :size], lambda: wide_v[j, :, size:], lambda: tall_v[j], None)


def mlp_pieces(u, acc, wide, tall):
    rows, dim = u.shape
    size = tall[0].shape[0]
    n = len(wide)
    vmem = pl.BlockSpec(memory_space=pltpu.VMEM)
    hbm = pl.BlockSpec(memory_space=pl.ANY)
    return pl.pallas_call(
        functools.partial(mlp_pieces_kernel, n),
        in_specs=[vmem, vmem] + [hbm] * (2 * n),
        out_specs=vmem,
        out_shape=jax.ShapeDtypeStruct((rows, dim), jnp.float32),
        scratch_shapes=[
            pltpu.VMEM((n, dim, 2 * size), jnp.bfloat16),
            pltpu.VMEM((n, size, dim), jnp.bfloat16),
            pltpu.SemaphoreType.DMA((2 * n,)),
        ],
        compiler_params=pltpu.CompilerParams(vmem_limit_bytes=56 * MIB),
        cost_estimate=cost(6 * rows * dim * size * n, 6 * dim * size * n + 10 * rows * dim),
    )(u, acc, *wide, *tall)


def solution(mesh):
    groups = mesh.shape['resp']
    row_axes = ('prompts', 'resp')
    head_spec = P(None, None, 'model', None)
    in_specs = (P(row_axes, None), P(row_axes, None, None), P(row_axes, None), P(row_axes), P(None, None), head_spec, head_spec, head_spec, P(None, 'model', None, None), P(None, None), P(None, None, 'model'), P(None, None, 'model'), P(None, 'model', None), P(None), P(None, 'model'))
    across = [(0, 1), (1, 0)]
    core = [(i, i ^ 1) for i in range(groups)]
    chip = [(i, i ^ 2) for i in range(groups)]
    both = [(i, i ^ 3) for i in range(groups)]

    def swap(a):
        return lax.ppermute(a, 'model', across)

    def spread(a):
        return [a, lax.ppermute(a, 'resp', core), lax.ppermute(a, 'resp', chip), lax.ppermute(a, 'resp', both)]

    def device_body(x_prompt, x_resp, targets, resp_lens, attn_gain, w_query, w_key, w_value, w_out, mlp_gain, w_gate, w_up, w_down, final_gain, w_vocab):
        me = lax.axis_index('resp')
        side = lax.axis_index('model')
        resp_len = x_resp.shape[1]
        dim = x_resp.shape[2]
        prompt_len = x_prompt.shape[0] * groups
        tokens = prompt_len + resp_len
        blocks = tokens // BLOCK
        key_rows = -(-tokens // 128) * 128
        q_width = w_query.shape[2] * HEAD
        ffn = w_gate.shape[2]
        vocab = w_vocab.shape[1]
        w_out = w_out.reshape(w_out.shape[0], q_width, dim)

        def in_order(pieces):
            stack = jnp.stack(pieces)
            return jnp.concatenate([lax.dynamic_index_in_dim(stack, me ^ j, 0, keepdims=False) for j in range(groups)], axis=0)

        def rows_of(w):
            size = w.shape[0] // groups
            return lax.dynamic_slice_in_dim(w, me * size, size, 0)

        def qkv(l, part):
            return jnp.concatenate([part(w_query[l]).reshape(-1, q_width), part(w_key[l]).reshape(-1, HEAD), part(w_value[l]).reshape(-1, HEAD)], axis=1)

        def fetch_rows(piece):
            return spread(swap(piece))

        qkv_far0 = in_order(fetch_rows(qkv(0, rows_of)))
        out_far0 = fetch_rows(rows_of(w_out[0]))
        qkv_far1 = fetch_rows(qkv(1, rows_of))
        out_far1 = fetch_rows(rows_of(w_out[1]))

        base = me * (sum(CHUNKS))
        wide, tall = [], []
        done = 0
        for c, size in enumerate(CHUNKS + (TAIL,)):
            if c < len(CHUNKS):
                at = base + done
            else:
                at = groups * done + jnp.minimum(me, (ffn - groups * done) // TAIL - 1) * TAIL
            w = jnp.concatenate([lax.dynamic_slice(w_gate, (1, 0, at), (1, dim, size))[0], lax.dynamic_slice(w_up, (1, 0, at), (1, dim, size))[0]], axis=1)
            t = lax.dynamic_slice(w_down, (1, at, 0), (1, size, dim))[0]
            if c == len(CHUNKS):
                t = jnp.where(me < (ffn - groups * done) // TAIL, t, jnp.zeros_like(t))
            w, t = swap(w), swap(t)
            wf, tf = lax.ppermute(w, 'resp', chip), lax.ppermute(t, 'resp', chip)
            wide.append([w, lax.ppermute(w, 'resp', core), wf, lax.ppermute(wf, 'resp', core)])
            tall.append([t, lax.ppermute(t, 'resp', core), tf, lax.ppermute(tf, 'resp', core)])
            done += size
        piece = vocab // groups
        vocab_far = spread(swap(lax.dynamic_slice_in_dim(w_vocab, me * piece, piece, 1)))

        prompt = in_order(spread(x_prompt))
        x = jnp.concatenate([prompt, x_resp[0]], axis=0)

        half = HEAD // 2
        frequency = ROPE_BASE ** (-jnp.arange(half, dtype=jnp.float32) / half)
        angles = jnp.arange(tokens).astype(jnp.float32)[:, None] * frequency
        cos_half, sin_half = jnp.cos(angles), jnp.sin(angles)
        cos_all = jnp.concatenate([cos_half, cos_half], axis=1)
        sin_all = jnp.concatenate([-sin_half, sin_half], axis=1)

        every = jnp.arange(blocks, dtype=jnp.int32)
        whole = lambda w: w
        q, k, v = project(every, x, attn_gain[0], qkv(0, whole), cos_all, sin_all, key_rows)
        mixed_own = attention(every, q, k, v, blocks)
        q, k, v = project(every, x, attn_gain[0], qkv_far0, cos_all, sin_all, key_rows)
        mixed_far = attention(every, q, k, v, blocks)
        q, out_far0 = lax.optimization_barrier((q, out_far0))
        out_far0 = in_order(out_far0)
        x, u = project_out(0, x, mixed_own, mixed_far, w_out, out_far0, mlp_gain[0])

        owned = jnp.array(OWNED, jnp.int32)
        mine = owned[side]
        theirs = owned[1 - side]
        per_side = len(OWNED[0])

        def take(a, ids):
            return jnp.concatenate([lax.dynamic_slice_in_dim(a, ids[i] * BLOCK, BLOCK, 0) for i in range(per_side)], axis=0)

        got = []
        for i in range(per_side):
            part = mlp_own(0, theirs[i:i + 1], u, BLOCK, w_gate, w_up, w_down)
            got.append(swap(part))
        zero = jnp.zeros((1,), jnp.int32)
        part_mine = mlp_own(0, zero, take(u, mine), per_side * BLOCK, w_gate, w_up, w_down)
        x = (take(x, mine).astype(jnp.float32) + (part_mine + jnp.concatenate(got, axis=0))).astype(jnp.bfloat16)

        x, qkv_far1 = lax.optimization_barrier((x, qkv_far1))
        qkv_far1 = in_order(qkv_far1)
        q_own, k_own, v_own = project(mine, x, attn_gain[1], qkv(1, whole), cos_all, sin_all, per_side * BLOCK)
        q_far, k_far, v_far = project(mine, x, attn_gain[1], qkv_far1, cos_all, sin_all, per_side * BLOCK)
        kv_mine = jnp.concatenate([k_own, v_own, k_far, v_far], axis=1)
        kv_sent = jnp.concatenate([k_far, v_far, k_own, v_own], axis=1)
        kv_got = swap(kv_sent)
        kv_mine, out_far1 = lax.optimization_barrier((kv_mine, out_far1))
        out_far1 = in_order(out_far1)

        def merge(own_part, far_part):
            def split(a):
                return [a[i * BLOCK:(i + 1) * BLOCK] for i in range(a.shape[0] // BLOCK)]

            a, b = split(own_part), split(far_part)
            order = [[None] * blocks, [None] * blocks]
            for s in range(2):
                for i, blk in enumerate(OWNED[s]):
                    order[s][blk] = a[i]
                for i, blk in enumerate(OWNED[1 - s]):
                    order[s][blk] = b[i]
            return jnp.concatenate([jnp.where(side == 0, p0, p1) for p0, p1 in zip(*order)], axis=0)

        kv = jnp.pad(merge(kv_mine, kv_got), ((0, key_rows - tokens), (0, 0)))
        mixed_own = attention(mine, q_own, kv[:, :HEAD], kv[:, HEAD:2 * HEAD], blocks)
        mixed_far = attention(mine, q_far, kv[:, 2 * HEAD:3 * HEAD], kv[:, 3 * HEAD:], blocks)
        x, u = project_out(1, x, mixed_own, mixed_far, w_out, out_far1, mlp_gain[1])
        total = mlp_own(1, zero, u, per_side * BLOCK, w_gate, w_up, w_down)
        for c in range(len(wide)):
            total = mlp_pieces(u, total, wide[c], tall[c])
        x = (x.astype(jnp.float32) + total).astype(jnp.bfloat16)

        logits = dot(normalize(x, final_gain), jnp.concatenate([w_vocab] + vocab_far, axis=1))
        ids = [side * vocab + jnp.arange(vocab)] + [(1 - side) * vocab + (me ^ j) * piece + jnp.arange(piece) for j in range(groups)]
        vocab_ids = jnp.concatenate(ids)
        padded_targets = jnp.concatenate([jnp.zeros((prompt_len,), targets.dtype), targets[0]])[:, None]
        target_own = take(padded_targets, mine)
        row_max = jnp.max(logits, axis=-1)
        exp_total = jnp.sum(jnp.exp(logits - row_max[:, None]), axis=-1)
        picked = jnp.sum(jnp.where(vocab_ids[None, :] == target_own, logits, 0.0), axis=-1)
        log_probs = picked - row_max - jnp.log(exp_total)
        log_probs = merge(log_probs, swap(log_probs))[prompt_len:]
        log_probs = jnp.where(jnp.arange(resp_len) < resp_lens[0], log_probs, 0.0)
        return log_probs[None, :]

    return jax.shard_map(device_body, mesh=mesh, in_specs=in_specs, out_specs=P(row_axes, None), check_vma=False)
```

```python
import functools
import math

import jax
import jax.numpy as jnp
import numpy as np
from jax import lax
from jax.experimental import pallas as pl
from jax.experimental.pallas import tpu as pltpu
from jax.sharding import PartitionSpec as P


EPS = 1e-6
ROPE_BASE = 10000.0
HEAD = 128
BLOCK = 352
TILE = 1024
SUB = 256
OWNED = ((0, 3, 5), (1, 2, 4))
CHUNKS = (256,) + (128,) * 6
CALLS = ((0,), (1, 2), (3, 4), (5, 6), (7,))
SPLIT = 2048
TAIL = 128
MIB = 2**20


def dot(a, b):
    return jnp.dot(a, b, preferred_element_type=jnp.float32)


def normalize(x, gain):
    f = x.astype(jnp.float32)
    inv_rms = lax.rsqrt(jnp.mean(f * f, axis=-1, keepdims=True) + EPS)
    return (f * inv_rms * gain).astype(jnp.bfloat16)


def params(vmem_mib):
    return pltpu.CompilerParams(dimension_semantics=("arbitrary",), vmem_limit_bytes=vmem_mib * MIB)


def cost(flops, data):
    return pl.CostEstimate(flops=int(flops), bytes_accessed=int(data), transcendentals=0)


def pack(jobs, shapes, *arrays):
    n = len(arrays)

    def kernel(*refs):
        srcs, dsts = refs[:n], refs[n:n + len(shapes)]
        stages, sems = refs[n + len(shapes):-1], refs[-1]
        me = lax.axis_index('resp')
        ins = []
        for t, (a, at, b, to) in enumerate(jobs):
            c = pltpu.make_async_copy(srcs[a].at[at(me)], stages[t], sems.at[2 * t])
            c.start()
            ins.append(c)
        outs = []
        for t, (a, at, b, to) in enumerate(jobs):
            ins[t].wait()
            c = pltpu.make_async_copy(stages[t], dsts[b].at[to], sems.at[2 * t + 1])
            c.start()
            outs.append(c)
        for c in outs:
            c.wait()

    out_shape = [jax.ShapeDtypeStruct(shape, jnp.bfloat16) for shape in shapes]
    sizes = [jax.eval_shape(lambda r, to=to: r[to], out_shape[b]).shape for _, _, b, to in jobs]
    hbm = pl.BlockSpec(memory_space=pltpu.HBM)
    return pl.pallas_call(
        kernel,
        in_specs=[hbm] * n,
        out_specs=[hbm] * len(shapes),
        out_shape=out_shape,
        scratch_shapes=[pltpu.VMEM(z, jnp.bfloat16) for z in sizes] + [pltpu.SemaphoreType.DMA((2 * len(jobs),))],
        compiler_params=pltpu.CompilerParams(vmem_limit_bytes=62 * MIB),
        cost_estimate=cost(10**9, 2 * sum(2 * o.size for o in out_shape)),
    )(*arrays)


def project_kernel(layer, far, q_heads, ids_ref, x_ref, gain_ref, far_turn_ref, near_turn_ref, *refs):
    w_refs, (q_ref, kv_ref, w_s) = refs[:-3], refs[-3:]

    @pl.when(pl.program_id(0) == 0)
    def _():
        if far:
            me = lax.axis_index('resp')
            for j, piece in enumerate(w_refs):
                size = piece.shape[1]
                at = pl.ds(pl.multiple_of((me ^ j) * size, size), size)
                for i in range(piece.shape[0]):
                    w_s[at, i * HEAD:(i + 1) * HEAD] = piece[i]
        else:
            for i in range(q_heads):
                w_s[:, i * HEAD:(i + 1) * HEAD] = w_refs[0][0, i]
            w_s[:, q_heads * HEAD:(q_heads + 1) * HEAD] = w_refs[1][0, 0]
            w_s[:, (q_heads + 1) * HEAD:] = w_refs[2][0, 0]

    h = normalize(x_ref[...], gain_ref[layer:layer + 1, :])
    f = dot(h, w_s[...])
    cos_a, sin_a = far_turn_ref[0, 0:1], far_turn_ref[0, 1:2]
    cos_b, sin_b = near_turn_ref[0], near_turn_ref[1]
    cos_part = cos_a * cos_b - sin_a * sin_b
    sin_part = sin_a * cos_b + cos_a * sin_b
    lane = lax.broadcasted_iota(jnp.int32, sin_part.shape, 1)
    sin_part = jnp.where(lane < HEAD // 2, -sin_part, sin_part)
    for i in range(q_heads + 1):
        a = f[:, i * HEAD:(i + 1) * HEAD]
        r = (a * cos_part + pltpu.roll(a, HEAD // 2, 1) * sin_part).astype(jnp.bfloat16)
        if i < q_heads:
            q_ref[:, i * HEAD:(i + 1) * HEAD] = r
        else:
            kv_ref[:, :HEAD] = r
    kv_ref[:, HEAD:] = f[:, (q_heads + 1) * HEAD:].astype(jnp.bfloat16)


def project(layer, ids, x, gain, ws, far, turns, key_rows):
    rows, dim = x.shape
    q_heads = ws[0].shape[0] - 2 if far else ws[0].shape[1]
    q_width = q_heads * HEAD
    width = q_width + 2 * HEAD
    row = lambda b, ids: (b, 0)
    if far:
        w_specs = [pl.BlockSpec(w.shape, lambda b, ids: (0, 0, 0)) for w in ws]
    else:
        w_specs = [pl.BlockSpec((1,) + w.shape[1:], lambda b, ids: (layer, 0, 0, 0)) for w in ws]
    return pl.pallas_call(
        functools.partial(project_kernel, layer, far, q_heads),
        grid_spec=pltpu.PrefetchScalarGridSpec(
            num_scalar_prefetch=1,
            grid=(rows // BLOCK,),
            in_specs=[
                pl.BlockSpec((BLOCK, dim), row),
                pl.BlockSpec(gain.shape, lambda b, ids: (0, 0)),
                pl.BlockSpec((1, 2, HEAD), lambda b, ids: (ids[b], 0, 0)),
                pl.BlockSpec((2, BLOCK, HEAD), lambda b, ids: (0, 0, 0)),
            ] + w_specs,
            out_specs=[pl.BlockSpec((BLOCK, q_width), row), pl.BlockSpec((BLOCK, 2 * HEAD), row)],
            scratch_shapes=[pltpu.VMEM((dim, width), jnp.bfloat16)],
        ),
        out_shape=[
            jax.ShapeDtypeStruct((rows, q_width), jnp.bfloat16),
            jax.ShapeDtypeStruct((key_rows, 2 * HEAD), jnp.bfloat16),
        ],
        compiler_params=params(40),
        cost_estimate=cost(2 * rows * dim * width, 2 * (rows * dim + dim * width + rows * width)),
    )(ids, x, gain, *turns, *ws)


def attention_kernel(num_blocks, heads, parts, ids_ref, q_ref, *refs):
    kvs = refs[:parts]
    o_ref, s0, s1, m0, m1 = refs[parts:parts + 5]
    step = pl.program_id(0)
    block_id = ids_ref[step]
    rows = q_ref.shape[0]
    nt = (((1,), (1,)), ((), ()))
    scale = HEAD ** -0.5 * math.log2(math.e)
    group = 512
    if parts == 1:
        kv_ref = kvs[0]
    else:
        kv_ref = refs[parts + 5]
        per = kvs[0].shape[0] // rows

        @pl.when(step == 0)
        def _():
            for p in range(parts):
                for i in range(per):
                    at = pl.ds(pl.multiple_of(ids_ref[p * per + i] * rows, rows), rows)
                    kv_ref[at, :] = kvs[p][i * rows:(i + 1) * rows, :]

    def body(i):
        first = i * rows
        low = first // 128 * 128
        high = -(-(first + rows) // 128) * 128
        cuts = [(low, high - low)] + [(c, min(group, low - c)) for c in range(0, low, group)]

        def columns(h):
            return pl.ds(pl.multiple_of(h * HEAD, HEAD), HEAD)

        def interleave(h_s, s_out, m_out, h_v, s_in, m_in):
            if h_s is not None:
                q = q_ref[:, columns(h_s)]
                top = None
            if h_v is not None:
                m = m_in[...]
                total, out = None, None
            for c, w in cuts:
                if h_s is not None:
                    s = lax.dot_general(q, kv_ref[c:c + w, :HEAD], nt, preferred_element_type=jnp.float32)
                    if c == low:
                        row = first + lax.broadcasted_iota(jnp.int32, s.shape, 0)
                        col = low + lax.broadcasted_iota(jnp.int32, s.shape, 1)
                        s = jnp.where(col <= row, s, -jnp.inf)
                    s_out[:, c:c + w] = s
                    for g in range(0, w, 128):
                        top = s[:, g:g + 128] if top is None else jnp.maximum(top, s[:, g:g + 128])
                if h_v is not None:
                    ps = []
                    for g in range(c, c + w, 128):
                        p = jnp.exp2((s_in[:, g:g + 128] - m) * scale)
                        total = p if total is None else total + p
                        ps.append(p.astype(jnp.bfloat16))
                    v = kv_ref[c:c + w, HEAD:]
                    if c + w > num_blocks * rows:
                        at = c + lax.broadcasted_iota(jnp.int32, v.shape, 0)
                        v = jnp.where(at < num_blocks * rows, v, jnp.zeros_like(v))
                    pv = dot(jnp.concatenate(ps, axis=1), v)
                    out = pv if out is None else out + pv
            if h_s is not None:
                m_out[...] = jnp.broadcast_to(jnp.max(top, axis=-1, keepdims=True), top.shape)
            if h_v is not None:
                o_ref[:, columns(h_v)] = (out / jnp.sum(total, axis=-1, keepdims=True)).astype(jnp.bfloat16)

        interleave(0, s0, m0, None, None, None)

        def pair(t, _):
            interleave(2 * t + 1, s1, m1, 2 * t, s0, m0)
            interleave(2 * t + 2, s0, m0, 2 * t + 1, s1, m1)
            return 0

        lax.fori_loop(0, heads // 2 - 1, pair, 0)
        interleave(heads - 1, s1, m1, heads - 2, s0, m0)
        interleave(None, None, None, heads - 1, s1, m1)

    for i in range(num_blocks):
        pl.when(block_id == i)(functools.partial(body, i))


def attention(ids, q, kvs, num_blocks, count, pick):
    rows, width = count * BLOCK, q.shape[1]
    keys = -(-num_blocks * BLOCK // 128) * 128
    scratch = [pltpu.VMEM((BLOCK, keys), jnp.float32)] * 2 + [pltpu.VMEM((BLOCK, HEAD), jnp.float32)] * 2
    if len(kvs) > 1:
        scratch.append(pltpu.VMEM((keys, 2 * HEAD), jnp.bfloat16))
    return pl.pallas_call(
        functools.partial(attention_kernel, num_blocks, width // HEAD, len(kvs)),
        grid_spec=pltpu.PrefetchScalarGridSpec(
            num_scalar_prefetch=1,
            grid=(rows // BLOCK,),
            in_specs=[pl.BlockSpec((BLOCK, width), lambda b, ids: (ids[b] if pick else b, 0))]
            + [pl.BlockSpec(kv.shape, lambda b, ids: (0, 0)) for kv in kvs],
            out_specs=pl.BlockSpec((BLOCK, width), lambda b, ids: (b, 0)),
            scratch_shapes=scratch,
        ),
        out_shape=jax.ShapeDtypeStruct((rows, width), jnp.bfloat16),
        compiler_params=params(40),
        cost_estimate=cost(8 * rows * keys * width, rows * width * 4 + keys * HEAD * 4),
    )(ids, q, *kvs)


def output_kernel(layer, ids_ref, x_ref, a_ref, b_ref, wa_ref, gain_ref, *refs):
    pieces, (x_out, u_out, w_s) = refs[:-3], refs[-3:]

    @pl.when(pl.program_id(0) == 0)
    def _():
        me = lax.axis_index('resp')
        for j, piece in enumerate(pieces):
            size = piece.shape[0]
            w_s[pl.ds(pl.multiple_of((me ^ j) * size, size), size), :] = piece[...]

    total = dot(a_ref[...], wa_ref[0]) + dot(b_ref[...], w_s[...])
    x = (x_ref[...].astype(jnp.float32) + total).astype(jnp.bfloat16)
    x_out[...] = x
    u_out[...] = normalize(x, gain_ref[layer:layer + 1, :])


def project_out(layer, ids, x, a, b, w_own, pieces, gain, pick):
    dim = x.shape[1]
    rows, width = a.shape
    row = lambda i, ids: (i, 0)
    return pl.pallas_call(
        functools.partial(output_kernel, layer),
        grid_spec=pltpu.PrefetchScalarGridSpec(
            num_scalar_prefetch=1,
            grid=(rows // BLOCK,),
            in_specs=[
                pl.BlockSpec((BLOCK, dim), lambda i, ids: (ids[i] if pick else i, 0)),
                pl.BlockSpec((BLOCK, width), row),
                pl.BlockSpec((BLOCK, width), row),
                pl.BlockSpec((1, width, dim), lambda i, ids: (layer, 0, 0)),
                pl.BlockSpec(gain.shape, lambda i, ids: (0, 0)),
            ] + [pl.BlockSpec(p.shape, lambda i, ids: (0, 0)) for p in pieces],
            out_specs=[pl.BlockSpec((BLOCK, dim), row), pl.BlockSpec((BLOCK, dim), row)],
            scratch_shapes=[pltpu.VMEM((width, dim), jnp.bfloat16)],
        ),
        out_shape=[jax.ShapeDtypeStruct((rows, dim), jnp.bfloat16)] * 2,
        compiler_params=params(40),
        cost_estimate=cost(4 * rows * dim * width, 6 * rows * dim + 8 * width * dim),
    )(ids, x, a, b, w_own, gain, *pieces)


def mlp_rows(u_ref, out_ref, row_tile, hidden, downs):
    def rows(i, _):
        at = pl.ds(pl.multiple_of(i * row_tile, row_tile), row_tile)
        u = u_ref[at, :]
        part = None
        for inner, down in zip(hidden(u), downs()):
            p = dot(inner, down)
            part = p if part is None else part + p
        out_ref[at, :] += part
        return 0

    n = u_ref.shape[0] // row_tile
    if n == 1:
        rows(0, 0)
    else:
        lax.fori_loop(0, n, rows, 0)


def gated(g, up):
    return (jax.nn.silu(g) * up).astype(jnp.bfloat16)


def mlp_kernel(columns, tile, ids_ref, u_ref, gate_ref, up_ref, down_ref, *refs):
    acc_ref, out_ref = refs if len(refs) == 2 else (None, refs[0])
    step = pl.program_id(0)
    steps = -(-columns // tile)

    @pl.when(step == 0)
    def _():
        out_ref[...] = jnp.zeros_like(out_ref) if acc_ref is None else acc_ref[...]

    def run(width):
        cuts = [(c, min(SUB, width - c)) for c in range(0, width, SUB)]

        def hidden(u):
            return [gated(dot(u, gate_ref[0, :, c:c + w]), dot(u, up_ref[0, :, c:c + w])) for c, w in cuts]

        mlp_rows(u_ref, out_ref, BLOCK, hidden, lambda: [down_ref[0, c:c + w, :] for c, w in cuts])

    pl.when(step < steps - 1)(lambda: run(tile))
    pl.when(step == steps - 1)(lambda: run(columns - (steps - 1) * tile))


def mlp_own(layer, ids, u, rows, tile, w_gate, w_up, w_down, acc=None, first=0, columns=None):
    dim = u.shape[1]
    columns = columns or w_gate.shape[2]
    skip = first // tile
    return pl.pallas_call(
        functools.partial(mlp_kernel, columns, tile),
        grid_spec=pltpu.PrefetchScalarGridSpec(
            num_scalar_prefetch=1,
            grid=(-(-columns // tile),),
            in_specs=[
                pl.BlockSpec((rows, dim), lambda j, ids: (ids[0], 0)),
                pl.BlockSpec((1, dim, tile), lambda j, ids: (layer, 0, skip + j)),
                pl.BlockSpec((1, dim, tile), lambda j, ids: (layer, 0, skip + j)),
                pl.BlockSpec((1, tile, dim), lambda j, ids: (layer, skip + j, 0)),
            ] + [pl.BlockSpec((rows, dim), lambda j, ids: (0, 0), pipeline_mode=pl.Buffered(1))] * (acc is not None),
            out_specs=pl.BlockSpec((rows, dim), lambda j, ids: (0, 0)),
        ),
        out_shape=jax.ShapeDtypeStruct((rows, dim), jnp.float32),
        compiler_params=params(60),
        cost_estimate=cost(6 * rows * dim * columns, 6 * dim * columns + 6 * rows * dim),
    )(ids, u, w_gate, w_up, w_down, *([] if acc is None else [acc]))


def log_prob_rows(x_ref, gain_ref, target_ref, vocab_refs, total):
    me, side = lax.axis_index('resp'), lax.axis_index('model')
    x = (x_ref[...].astype(jnp.float32) + total).astype(jnp.bfloat16)
    h = normalize(x, gain_ref[...])
    target = target_ref[...]
    parts = [dot(h, w[...]) for w in vocab_refs]
    top = None
    picked = 0.0
    for j, logits in enumerate(parts):
        width = logits.shape[1]
        own = vocab_refs[0].shape[1]
        first = side * own if j == 0 else (1 - side) * own + (me ^ (j - 1)) * width
        ids = first + lax.broadcasted_iota(jnp.int32, logits.shape, 1)
        picked = picked + jnp.sum(jnp.where(ids == target, logits, 0.0), axis=-1, keepdims=True)
        m = jnp.max(logits, axis=-1, keepdims=True)
        top = m if top is None else jnp.maximum(top, m)
    exp_total = sum(jnp.sum(jnp.exp(logits - top), axis=-1, keepdims=True) for logits in parts)
    return picked - top - jnp.log(exp_total)


def mlp_pieces_kernel(counts, sizes, tail_blocks, has_acc, head, u_ref, *refs):
    n = sum(counts)
    acc_ref, refs = (refs[0], refs[1:]) if has_acc else (None, refs)
    head_refs, refs = refs[:head], refs[head:]
    wide, tall = refs[:n], refs[n:2 * n]
    out_ref, wide_s, tall_s, sems = refs[2 * n], refs[2 * n + 1:3 * n + 1], refs[-2], refs[-1]
    kinds = [k for k, count in enumerate(counts) for _ in range(count)]
    me = lax.axis_index('resp')

    @pl.when(pl.program_id(0) == 0)
    def _():
        copies = []
        at = 0
        for j, k in enumerate(kinds):
            for i, (src, dst) in enumerate(((wide[j], wide_s[j]), (tall[j], tall_s.at[at:at + sizes[k]]))):
                c = pltpu.make_async_copy(src, dst, sems.at[2 * j + i])
                c.start()
                copies.append(c)
            at += sizes[k]
        for c in copies:
            c.wait()

    u = u_ref[...]
    parts = []
    for j, k in enumerate(kinds):
        f = dot(u, wide_s[j][...])
        inner = gated(f[:, :sizes[k]], f[:, sizes[k]:])
        if tail_blocks and k == len(counts) - 1:
            inner = jnp.where((me ^ (j - sum(counts[:k]))) < tail_blocks, inner, jnp.zeros_like(inner))
        parts.append(inner)
    total = dot(jnp.concatenate(parts, axis=1), tall_s[...])
    if acc_ref is not None:
        total = acc_ref[...] + total
    out_ref[...] = log_prob_rows(*head_refs[:3], head_refs[3:], total) if head else total


def mlp_pieces(u, acc, wides, talls, tail_blocks, head):
    rows, dim = u.shape
    counts = [len(w) for w in wides]
    sizes = [t[0].shape[0] for t in talls]
    wide = [p for w in wides for p in w]
    tall = [p for t in talls for p in t]
    n = len(wide)
    row = lambda i: (i, 0)
    hbm = pl.BlockSpec(memory_space=pltpu.HBM)
    hidden = sum(p.shape[0] for p in tall)
    return pl.pallas_call(
        functools.partial(mlp_pieces_kernel, counts, sizes, tail_blocks, acc is not None, len(head)),
        grid=(rows // BLOCK,),
        in_specs=[pl.BlockSpec((BLOCK, dim), row)] * (1 if acc is None else 2)
        + [pl.BlockSpec((BLOCK if a.shape[0] == rows else a.shape[0], a.shape[1]), row if a.shape[0] == rows else lambda i: (0, 0)) for a in head]
        + [hbm] * (2 * n),
        out_specs=pl.BlockSpec((BLOCK, 1 if head else dim), row),
        out_shape=jax.ShapeDtypeStruct((rows, 1 if head else dim), jnp.float32),
        scratch_shapes=[pltpu.VMEM(p.shape, jnp.bfloat16) for p in wide]
        + [pltpu.VMEM((hidden, dim), jnp.bfloat16), pltpu.SemaphoreType.DMA((2 * n,))],
        compiler_params=params(48),
        cost_estimate=cost(6 * rows * dim * hidden, 6 * dim * hidden + 10 * rows * dim),
    )(u, *([] if acc is None else [acc]), *head, *wide, *tall)


def solution(mesh):
    groups = mesh.shape['resp']
    row_axes = ('prompts', 'resp')
    head_spec = P(None, None, 'model', None)
    in_specs = (P(row_axes, None), P(row_axes, None, None), P(row_axes, None), P(row_axes), P(None, None), head_spec, head_spec, head_spec, P(None, 'model', None, None), P(None, None), P(None, None, 'model'), P(None, None, 'model'), P(None, 'model', None), P(None), P(None, 'model'))
    across = [(0, 1), (1, 0)]
    core = [(i, i ^ 1) for i in range(groups)]
    chip = [(i, i ^ 2) for i in range(groups)]
    both = [(i, i ^ 3) for i in range(groups)]

    def swap(a):
        return lax.ppermute(a, 'model', across)

    def spread(a):
        return [a, lax.ppermute(a, 'resp', core), lax.ppermute(a, 'resp', chip), lax.ppermute(a, 'resp', both)]

    def device_body(x_prompt, x_resp, targets, resp_lens, attn_gain, w_query, w_key, w_value, w_out, mlp_gain, w_gate, w_up, w_down, final_gain, w_vocab):
        me = lax.axis_index('resp')
        side = lax.axis_index('model')
        resp_len = x_resp.shape[1]
        dim = x_resp.shape[2]
        prompt_len = x_prompt.shape[0] * groups
        tokens = prompt_len + resp_len
        blocks = tokens // BLOCK
        key_rows = -(-tokens // 128) * 128
        q_width = w_query.shape[2] * HEAD
        ffn = w_gate.shape[2]
        vocab = w_vocab.shape[1]
        w_out = w_out.reshape(w_out.shape[0], q_width, dim)
        w_query = jnp.transpose(w_query, (0, 2, 1, 3))
        w_key = jnp.transpose(w_key, (0, 2, 1, 3))
        w_value = jnp.transpose(w_value, (0, 2, 1, 3))
        q_heads = q_width // HEAD
        own_qkv = (w_query, w_key, w_value)

        def in_order(pieces):
            stack = jnp.stack(pieces)
            return jnp.concatenate([lax.dynamic_index_in_dim(stack, me ^ j, 0, keepdims=False) for j in range(groups)], axis=0)

        every_row = slice(None)
        r_in, r_out, piece = dim // groups, q_width // groups, vocab // groups

        def attention_jobs(l, first):
            rows_in = lambda me: pl.ds(me * r_in, r_in)
            return [
                (0, lambda me: (l, every_row, rows_in(me), every_row), first, (slice(0, q_heads),)),
                (1, lambda me: (l, every_row, rows_in(me), every_row), first, (slice(q_heads, q_heads + 1),)),
                (2, lambda me: (l, every_row, rows_in(me), every_row), first, (slice(q_heads + 1, q_heads + 2),)),
                (3, lambda me: (l, pl.ds(me * r_out, r_out), every_row), first + 1, (slice(None),)),
            ]

        attention_shapes = [(q_heads + 2, r_in, HEAD), (r_out, dim)]
        qkv0, out0 = pack(attention_jobs(0, 0), attention_shapes, *own_qkv, w_out)
        jobs = attention_jobs(1, 0) + [(7, lambda me: (every_row, pl.ds(me * piece, piece)), 2, (slice(None),))]
        shapes = attention_shapes + [(dim, piece)]
        main = sum(CHUNKS)
        tail_blocks = (ffn - groups * main) // TAIL
        done = 0
        for c, size in enumerate(CHUNKS + (TAIL,)):
            if c < len(CHUNKS):
                at = lambda me, done=done: pl.multiple_of(me * main + done, 128)
            else:
                at = lambda me: pl.multiple_of(groups * main + jnp.minimum(me, tail_blocks - 1) * TAIL, 128)
            n = len(shapes)
            jobs += [
                (4, lambda me, at=at, size=size: (1, every_row, pl.ds(at(me), size)), n, (every_row, slice(0, size))),
                (5, lambda me, at=at, size=size: (1, every_row, pl.ds(at(me), size)), n, (every_row, slice(size, 2 * size))),
                (6, lambda me, at=at, size=size: (1, pl.ds(at(me), size), every_row), n + 1, (every_row,)),
            ]
            shapes += [(dim, 2 * size), (size, dim)]
            done += size
        qkv0_y = swap(qkv0)
        qkv1, out1, voc, *chunks = pack(jobs, shapes, *own_qkv, w_out, w_gate, w_up, w_down, w_vocab)

        qkv_far0 = spread(qkv0_y)
        out_far0 = spread(swap(out0))
        qkv_far1 = spread(swap(qkv1))
        out_far1 = spread(swap(out1))
        vocab_far = spread(swap(voc))
        wide, tall = [], []
        for c in range(len(chunks) // 2):
            w, t = swap(chunks[2 * c]), swap(chunks[2 * c + 1])
            wf, tf = lax.ppermute(w, 'resp', chip), lax.ppermute(t, 'resp', chip)
            wide.append([w, lax.ppermute(w, 'resp', core), wf, lax.ppermute(wf, 'resp', core)])
            tall.append([t, lax.ppermute(t, 'resp', core), tf, lax.ppermute(tf, 'resp', core)])

        prompt = in_order(spread(x_prompt))
        x = jnp.concatenate([prompt, x_resp[0]], axis=0)

        half = HEAD // 2
        frequency = (ROPE_BASE ** (-(np.arange(HEAD) % half) / half)).astype(np.float32)

        def turn(positions, axis):
            angles = positions.astype(np.float32)[:, None] * frequency
            return jnp.asarray(np.stack([np.cos(angles), np.sin(angles)], axis=axis))

        turns = (turn(np.arange(blocks) * BLOCK, 1), turn(np.arange(BLOCK), 0))

        every = jnp.arange(blocks, dtype=jnp.int32)
        owned = jnp.array(OWNED, jnp.int32)
        mine = owned[side]
        theirs = owned[1 - side]
        per_side = len(OWNED[0])
        q_own, kv_own = project(0, every, x, attn_gain, own_qkv, False, turns, key_rows)
        a = attention(theirs, q_own, [kv_own], blocks, per_side, True)
        q_far, kv_far = project(0, every, x, attn_gain, qkv_far0, True, turns, key_rows)
        b = attention(theirs, q_far, [kv_far], blocks, per_side, True)
        _, u = project_out(0, theirs, x, a, b, w_out, out_far0, mlp_gain, True)
        got = []
        for i in range(per_side):
            part = mlp_own(0, jnp.full((1,), i, jnp.int32), u, BLOCK, 512, w_gate, w_up, w_down)
            got.append(swap(part))
        a = attention(mine, q_own, [kv_own], blocks, per_side, True)
        b = attention(mine, q_far, [kv_far], blocks, per_side, True)
        x, u = project_out(0, mine, x, a, b, w_out, out_far0, mlp_gain, True)
        zero = jnp.zeros((1,), jnp.int32)
        part_mine = mlp_own(0, zero, u, per_side * BLOCK, TILE, w_gate, w_up, w_down)
        x = (x.astype(jnp.float32) + (part_mine + jnp.concatenate(got, axis=0))).astype(jnp.bfloat16)

        q_far, kv_far = project(1, mine, x, attn_gain, qkv_far1, True, turns, per_side * BLOCK)
        got_own = swap(kv_far)
        q_own, kv_own = project(1, mine, x, attn_gain, own_qkv, False, turns, per_side * BLOCK)
        got_far = swap(kv_own)

        def merge(own_part, far_part):
            def split(a):
                return [a[i * BLOCK:(i + 1) * BLOCK] for i in range(a.shape[0] // BLOCK)]

            a, b = split(own_part), split(far_part)
            order = [[None] * blocks, [None] * blocks]
            for s in range(2):
                for i, blk in enumerate(OWNED[s]):
                    order[s][blk] = a[i]
                for i, blk in enumerate(OWNED[1 - s]):
                    order[s][blk] = b[i]
            return jnp.concatenate([jnp.where(side == 0, p0, p1) for p0, p1 in zip(*order)], axis=0)

        mine_first = jnp.concatenate([mine, theirs])
        mixed_own = attention(mine_first, q_own, [kv_own, got_own], blocks, per_side, False)
        mixed_far = attention(mine_first, q_far, [kv_far, got_far], blocks, per_side, False)
        x, u = project_out(1, mine, x, mixed_own, mixed_far, w_out, out_far1, mlp_gain, False)
        padded_targets = jnp.concatenate([jnp.zeros((prompt_len,), targets.dtype), targets[0]]).reshape(blocks, BLOCK)
        target_own = jnp.concatenate([lax.dynamic_index_in_dim(padded_targets, mine[i], 0, keepdims=False) for i in range(per_side)])[:, None]
        total = None
        for n, call in enumerate(CALLS):
            if n == 1:
                total = mlp_own(1, zero, u, per_side * BLOCK, TILE, w_gate, w_up, w_down, total, 0, SPLIT)
            if n == 2:
                total = mlp_own(1, zero, u, per_side * BLOCK, TILE, w_gate, w_up, w_down, total, SPLIT, ffn - SPLIT)
            head = (x, final_gain[None, :], target_own, w_vocab, *vocab_far) if n == len(CALLS) - 1 else ()
            total = mlp_pieces(u, total, [wide[c] for c in call], [tall[c] for c in call], tail_blocks if len(CHUNKS) in call else 0, head)
        log_probs = total[:, 0]
        log_probs = merge(log_probs, swap(log_probs))[prompt_len:]
        log_probs = jnp.where(jnp.arange(resp_len) < resp_lens[0], log_probs, 0.0)
        return log_probs[None, :]

    return jax.shard_map(device_body, mesh=mesh, in_specs=in_specs, out_specs=P(row_axes, None), check_vma=False)
```
